32 devices in a mesh: frag: 2 (over x), occ: 2 (over core), vir: 8 (over z, y).
Axes of the slice: x: 2, y: 2, z: 4, core: 2. Of those that a mesh axis runs over, the one named last changes fastest.
Arguments:
- factors: bfloat16 [8, 1024, 3072], P(('frag', 'occ'), 'vir'), parts along dimension 0, may hold values from -2 to 2
- occ_energy: int32 [8], P('frag'), parts along dimension 0, may hold values from -1536 to -512
- vir_energy: int32 [2048], P('frag'), parts along dimension 0, may hold values from 512 to 4096
Outputs:
- density: float32 [8, 1024, 3072], P(('frag', 'occ'), 'vir'), parts along dimension 0
The draws below stay inside these ranges and needn't reach their ends.
There are 2 independent parts, one for each index of `frag`. The reference program is written for one: setup_inputs(seed, part) draws one part's arguments, and reference() takes and returns one part's arrays. A program takes and returns all parts, laid end to end along the dimension named above; each array names one. Nothing has to cross between parts.
Inputs may be any that keep to these rules, and one draw needn't show every extreme that they name: `occ_energy`: occupied energies lie at or below the highest occupied level -512. `vir_energy`: virtual energies lie at or above the lowest virtual level 512.
All inputs are finite; a program needn't handle non-finite values.
Results may differ from the reference program's by a relative error of at most 0.0055.
Values may be sent and summed in bfloat16 or wider, within the bound.
No kernel may reach another device: no remote copies, remote signals or barrier semaphores. Data moves between devices by JAX's collectives and lax.ppermute only.
A program may use at most 128 MiB of HBM per device.

```python
import jax
import jax.numpy as jnp
from jax import lax

V = 1024
NAUX = 3072
OCC = 4


def place_ends(entries, key, smallest, high):
    index_at = [jax.random.randint(jax.random.fold_in(key, axis), (), 0, length) for axis, length in enumerate(entries.shape)]
    longest = entries.shape.index(max(entries.shape))
    next_to = index_at[:longest] + [(index_at[longest] + 1) % entries.shape[longest]] + index_at[longest + 1:]
    return entries.at[tuple(index_at)].set(smallest).at[tuple(next_to)].set(high)


def block_scale(stream_key, extent, cuts, low, high):
    loudness = 1.0
    for dim, shards_of in cuts:
        draws = jax.random.uniform(jax.random.fold_in(jax.random.fold_in(stream_key, 6), dim), (shards_of,), jnp.float32, low / len(cuts), high / len(cuts))
        loudness = loudness * jnp.repeat(jnp.exp(draws), extent[dim] // shards_of).reshape((-1,) + (1,) * (len(extent) - 1 - dim))
    return loudness


def noise(key, shape, deviation, most, cuts=(), kind=jnp.bfloat16):
    result = deviation * jax.random.normal(key, shape, jnp.float32)
    if cuts:
        result = result * block_scale(key, shape, cuts, -0.22, 0.18)
    return jnp.clip(result, -most, most).astype(kind)


def setup_inputs(seed: int = 0, part: int = 0) -> dict:
    arg_keys = jax.random.split(jax.random.key(seed), 4)
    part_keys = jax.random.split(jax.random.fold_in(arg_keys[3], part), 4)
    factors = noise(part_keys[0], (OCC, V, NAUX), 0.134, 2.0, ((0, 2), (1, 8)))
    occ_energy = place_ends(jax.random.randint(part_keys[1], (OCC,), -1536, -511), jax.random.fold_in(part_keys[1], 1), -1536, (-511) - 1).astype(jnp.int32)
    vir_energy = place_ends(jax.random.randint(part_keys[2], (V,), 512, 4097), jax.random.fold_in(part_keys[2], 1), 512, 4096).astype(jnp.int32)
    return dict(factors=factors, occ_energy=occ_energy, vir_energy=vir_energy)


energy_unit = 1.0 / 1024.0


def pair_density(factors, occ_energy, vir_energy, i):
    own = lax.dynamic_index_in_dim(factors, i, 0, keepdims=False)

    def step(j, acc):
        partner = lax.dynamic_index_in_dim(factors, j, 0, keepdims=False)
        direct = jnp.dot(own, partner.T, preferred_element_type=jnp.float32).astype(jnp.bfloat16)
        crossed = direct.T
        divisor = (occ_energy[i] + occ_energy[j] - vir_energy[:, None] - vir_energy[None, :]).astype(jnp.float32) * energy_unit
        amplitude = ((2.0 * direct.astype(jnp.float32) - crossed.astype(jnp.float32)) / divisor).astype(jnp.bfloat16)
        return acc + jnp.dot(amplitude, partner, preferred_element_type=jnp.float32)

    return lax.fori_loop(0, OCC, step, jnp.zeros((V, NAUX), jnp.float32))


def reference(factors, occ_energy, vir_energy):
    return lax.map(lambda i: pair_density(factors, occ_energy, vir_energy, i), jnp.arange(OCC, dtype=jnp.int32))
```

```python
import functools

import jax
import jax.numpy as jnp
from jax import lax
from jax.experimental import pallas as pl
from jax.experimental.pallas import tpu as pltpu
from jax.sharding import PartitionSpec as P

energy_unit = 1.0 / 1024.0


across = (((1,), (1,)), ((), ()))
along = (((1,), (0,)), ((), ()))


def ring_order(mesh, axis):
    devices = mesh.devices
    for name in reversed(mesh.axis_names):
        if name != axis:
            devices = devices[(slice(None),) * mesh.axis_names.index(name) + (0,)]
    count = len(devices)
    spots = [tuple(getattr(device, "coords", ())) for device in devices]
    widths = [len(set(values)) for values in zip(*spots)] if all(spots) else []
    if sorted(widths)[-2:-1] == [2] and sorted(widths)[-1] * 2 == count:
        long = max(range(len(widths)), key=lambda d: widths[d])
        short = [d for d in range(len(widths)) if widths[d] == 2 and d != long][0]
        low = min(spot[short] for spot in spots)
        there = sorted((k for k in range(count) if spots[k][short] == low), key=lambda k: spots[k][long])
        back = sorted((k for k in range(count) if spots[k][short] != low), key=lambda k: -spots[k][long])
        return there + back
    return list(range(count))


def block_kernel(number, parts, local, where, occ_energy, own_vir, vir_energy, *refs):
    own = refs[:parts]
    pieces = refs[parts : parts + parts * local]
    out = refs[-1]
    prior = refs[-2] if len(refs) > parts + parts * local + 1 else None
    rows, aux = pieces[0].shape
    me = where[0]
    total = parts * local

    def product(left, right):
        return lax.dot_general(left, right, across, preferred_element_type=jnp.float32).astype(jnp.bfloat16)

    direct = [[product(own[0][i], pieces[j][...]) for j in range(total)] for i in range(local)]
    swapped = [
        [direct[j][i] if j < local else product(own[j // local][j % local], pieces[i][...]) for j in range(total)]
        for i in range(local)
    ]
    vir_row = vir_energy[where[1 + number]]
    vir_pair = own_vir[...] + vir_row

    def energy(k):
        return occ_energy[lax.rem(me * local + k, total)]

    for i in range(local):
        amplitudes = []
        for j in range(total):
            divisor = (energy(i) + energy(j) - vir_pair).astype(jnp.float32) * energy_unit
            top = 2.0 * direct[i][j].astype(jnp.float32) - swapped[i][j].astype(jnp.float32)
            amplitudes.append((top / divisor).astype(jnp.bfloat16))
        sum_here = None
        for j in range(total):
            term = lax.dot_general(amplitudes[j], pieces[j][...], along, preferred_element_type=jnp.float32)
            sum_here = term if sum_here is None else sum_here + term
        out[i] = sum_here if prior is None else prior[i] + sum_here


def block_step(number, parts, where, occ_energy, own_vir, vir_energy, own, pieces, density):
    local, rows, aux = own[0].shape
    vmem = pl.BlockSpec(memory_space=pltpu.VMEM)
    smem = pl.BlockSpec(memory_space=pltpu.SMEM)
    operands = [where, occ_energy, own_vir, vir_energy, *own, *pieces]
    specs = [smem, smem] + [vmem] * (len(operands) - 2)
    aliases = {}
    if density is not None:
        aliases = {len(operands): 0}
        operands.append(density)
        specs.append(vmem)
    total = parts * local
    products = local * total * 2 + local * (total - local)
    return pl.pallas_call(
        functools.partial(block_kernel, number, parts, local),
        out_shape=jax.ShapeDtypeStruct((local, rows, aux), jnp.float32),
        in_specs=specs,
        out_specs=vmem,
        input_output_aliases=aliases,
        compiler_params=pltpu.CompilerParams(vmem_limit_bytes=40 * 1024 * 1024),
        cost_estimate=pl.CostEstimate(
            flops=2 * products * rows * rows * aux,
            bytes_accessed=2 * (total * 2 + local * 4) * rows * aux,
            transcendentals=0,
        ),
        name=f"block_{number}",
    )(*operands)


def on_device(order, parts, factors, occ_energy, vir_energy):
    local, rows, aux = factors.shape
    count = len(order)
    core = lax.axis_index("occ")
    place = lax.axis_index("vir")
    onward = [(order[k], order[(k + 1) % count]) for k in range(count)]
    backward = [(target, source) for source, target in onward]
    spots = [order.index(k) for k in range(count)]
    spot = jnp.asarray(spots, jnp.int32)[place]

    def from_cores(piece):
        return [
            lax.ppermute(piece, "occ", [((k + shift) % parts, k) for k in range(parts)]) for shift in range(1, parts)
        ]

    first = [factors[k] for k in range(local)]
    half = local // 2
    behind, ahead = {}, {}
    carry_on, carry_back = first, first
    far = count // 2
    for distance in range(1, far + 1):
        last = distance == far and count % 2 == 0
        keep_on = range(0, half) if last else range(local)
        keep_back = range(half, local) if last else range(local)
        carry_on = {k: lax.ppermute(carry_on[k], "vir", onward) for k in keep_on}
        carry_back = {k: lax.ppermute(carry_back[k], "vir", backward) for k in keep_back}
        if last:
            behind[distance] = {**carry_on, **carry_back}
        else:
            behind[distance] = carry_on
            ahead[distance] = carry_back
    visits = [(0, {k: first[k] for k in range(local)})]
    for distance in range(1, far + 1):
        visits.append((-distance, behind[distance]))
        if distance in ahead:
            visits.append((distance, ahead[distance]))

    shifts = jnp.asarray([shift for shift, _ in visits], jnp.int32)
    sources = jnp.asarray(order, jnp.int32)[lax.rem(spot + shifts + count, count)]
    where = jnp.concatenate([core[None].astype(jnp.int32), sources])
    vir_table = vir_energy.reshape(count, 1, rows)
    own_vir = lax.dynamic_slice_in_dim(vir_energy, place * rows, rows)[:, None]
    own = [factors] + from_cores(factors)

    density = None
    for number, (_, pieces) in enumerate(visits):
        mine = [pieces[k] for k in range(local)]
        if number == 0:
            theirs = [block[k] for block in own[1:] for k in range(local)]
        else:
            moved = [from_cores(piece) for piece in mine]
            theirs = [moved[k][shift] for shift in range(parts - 1) for k in range(local)]
        density = block_step(
            number, parts, where, occ_energy, own_vir, vir_table, own, mine + theirs, density
        )
    return density


def solution(mesh):
    return jax.shard_map(
        functools.partial(on_device, ring_order(mesh, "vir"), mesh.shape["occ"]),
        mesh=mesh,
        in_specs=(P(("frag", "occ"), "vir", None), P("frag"), P("frag")),
        out_specs=P(("frag", "occ"), "vir", None),
        check_vma=False,
    )
```

```python
import functools

import jax
import jax.numpy as jnp
from jax import lax
from jax.experimental import pallas as pl
from jax.experimental.pallas import tpu as pltpu
from jax.sharding import PartitionSpec as P

energy_unit = 1.0 / 1024.0


across = (((1,), (1,)), ((), ()))
along = (((1,), (0,)), ((), ()))


def ring_order(mesh, axis):
    devices = mesh.devices
    for name in reversed(mesh.axis_names):
        if name != axis:
            devices = devices[(slice(None),) * mesh.axis_names.index(name) + (0,)]
    count = len(devices)
    spots = [tuple(getattr(device, "coords", ())) for device in devices]
    widths = [len(set(values)) for values in zip(*spots)] if all(spots) else []
    if sorted(widths)[-2:-1] == [2] and sorted(widths)[-1] * 2 == count:
        long = max(range(len(widths)), key=lambda d: widths[d])
        short = [d for d in range(len(widths)) if widths[d] == 2 and d != long][0]
        low = min(spot[short] for spot in spots)
        there = sorted((k for k in range(count) if spots[k][short] == low), key=lambda k: spots[k][long])
        back = sorted((k for k in range(count) if spots[k][short] != low), key=lambda k: -spots[k][long])
        return there + back
    return list(range(count))


def block_kernel(number, parts, local, steps, prior, where, occ_energy, own_vir, vir_energy, *refs):
    own = refs[:parts]
    pieces = refs[parts : parts + parts * local]
    direct, amplitude, density, out_sem, in_sem = refs[-5:]
    out = refs[-6]
    rows, aux = pieces[0].shape
    tiles = in_sem.shape[0]
    step = aux // tiles
    me = where[0]
    total = parts * local
    wide = local * rows

    def tile_copy(start, inward):
        columns = pl.ds(pl.multiple_of(start * step, step), step)
        if inward:
            return pltpu.make_async_copy(refs[-7].at[:, :, columns], density.at[:, :, columns], in_sem.at[start])
        return pltpu.make_async_copy(density.at[:, :, columns], out.at[:, :, columns], out_sem.at[start])

    if prior:
        for start in range(tiles):
            tile_copy(start, True).start()

    def stack(arrays):
        return jnp.concatenate(arrays, axis=0) if len(arrays) > 1 else arrays[0]

    def depth_step(k, carry):
        columns = pl.ds(pl.multiple_of(k * depth, depth), depth)
        all_rows = stack([block[:, :, columns].reshape(wide, depth) for block in own])
        for part in range(parts):
            left = all_rows if part == 0 else all_rows[:wide]
            right = stack([piece[:, columns] for piece in pieces[part * local : (part + 1) * local]])
            term = lax.dot_general(left, right, across, preferred_element_type=jnp.float32)
            at = pl.ds(0 if part == 0 else (parts + part - 1) * wide, left.shape[0])
            direct[at, :] = direct[at, :] + term
        return carry

    direct[...] = jnp.zeros_like(direct)
    depth = aux // steps
    lax.fori_loop(0, steps, depth_step, 0)
    vir_row = vir_energy[where[1 + number]]
    vir_pair = own_vir[...] + vir_row

    def energy(k):
        return occ_energy[lax.rem(me * local + k, total)]

    def tile(row, column):
        sums = direct[row * rows : (row + 1) * rows, column * rows : (column + 1) * rows]
        return sums.astype(jnp.bfloat16).astype(jnp.float32)

    for i in range(local):
        for j in range(total):
            part = j // local
            divisor = (energy(i) + energy(j) - vir_pair).astype(jnp.float32) * energy_unit
            straight = tile(i if part == 0 else (parts + part - 1) * local + i, j % local)
            top = 2.0 * straight - tile(j, i)
            amplitude[i * rows : (i + 1) * rows, j * rows : (j + 1) * rows] = (top / divisor).astype(jnp.bfloat16)

    def tile_step(start, carry):
        columns = pl.ds(pl.multiple_of(start * step, step), step)
        factor = stack([piece[:, columns] for piece in pieces])
        term = lax.dot_general(amplitude[...], factor, along, preferred_element_type=jnp.float32)
        term = term.reshape(local, rows, step)
        if prior:
            tile_copy(start, True).wait()
            term = density[:, :, columns] + term
        density[:, :, columns] = term
        tile_copy(start, False).start()
        return carry

    lax.fori_loop(0, tiles, tile_step, 0)
    for start in range(tiles):
        tile_copy(start, False).wait()


def block_step(number, parts, where, occ_energy, own_vir, vir_energy, own, pieces, density):
    local, rows, aux = own[0].shape
    vmem = pl.BlockSpec(memory_space=pltpu.VMEM)
    smem = pl.BlockSpec(memory_space=pltpu.SMEM)
    hbm = pl.BlockSpec(memory_space=pltpu.HBM)
    operands = [where, occ_energy, own_vir, vir_energy, *own, *pieces]
    specs = [smem, smem] + [vmem] * (len(operands) - 2)
    aliases = {}
    if density is not None:
        aliases = {len(operands): 0}
        operands.append(density)
        specs.append(hbm)
    total = parts * local
    products = local * total * 2 + local * (total - local)
    tiles = max(k for k in range(1, 7) if aux % (128 * k) == 0)
    steps = max(k for k in range(1, 5) if aux % (128 * k) == 0)
    wide = local * rows
    return pl.pallas_call(
        functools.partial(block_kernel, number, parts, local, steps, density is not None),
        out_shape=jax.ShapeDtypeStruct((local, rows, aux), jnp.float32),
        in_specs=specs,
        out_specs=hbm,
        scratch_shapes=[
            pltpu.VMEM(((2 * parts - 1) * wide, wide), jnp.float32),
            pltpu.VMEM((wide, parts * wide), jnp.bfloat16),
            pltpu.VMEM((local, rows, aux), jnp.float32),
            pltpu.SemaphoreType.DMA((tiles,)),
            pltpu.SemaphoreType.DMA((tiles,)),
        ],
        input_output_aliases=aliases,
        compiler_params=pltpu.CompilerParams(vmem_limit_bytes=24 * 1024 * 1024),
        cost_estimate=pl.CostEstimate(
            flops=2 * products * rows * rows * aux,
            bytes_accessed=2 * (total * 2 + local * 4) * rows * aux,
            transcendentals=0,
        ),
    )(*operands)


def plan(count, local):
    far = count // 2
    split = count % 2 == 0
    half = local // 2
    steps = [[], []]
    blocks = [(0, 0, 0)]
    for distance in range(1, far + 1):
        last = split and distance == far
        steps[0] += [(distance, k) for k in (range(0, half) if last else range(local))]
        steps[1] += [(distance, k) for k in reversed(range(half, local) if last else range(local))]
        blocks.append((distance, 0, len(steps[0])))
        if not last:
            blocks.append((distance, 1, len(steps[0])))
    return steps, blocks


def on_device(order, parts, factors, occ_energy, vir_energy):
    local, rows, _ = factors.shape
    count = len(order)
    core = lax.axis_index("occ")
    place = lax.axis_index("vir")
    onward = [(order[k], order[(k + 1) % count]) for k in range(count)]
    backward = [(target, source) for source, target in onward]
    links = (onward, backward)
    spots = [order.index(k) for k in range(count)]
    spot = jnp.asarray(spots, jnp.int32)[place]
    steps, blocks = plan(count, local)

    def from_cores(piece):
        return [
            lax.ppermute(piece, "occ", [((k + shift) % parts, k) for k in range(parts)])
            for shift in range(1, parts)
        ]

    held = [{(0, k): factors[k] for k in range(local)} for _ in links]
    near = [{}, {}]
    own = [factors] + from_cores(factors)
    for number in range(len(steps[0])):
        for way in range(2):
            distance, k = steps[way][number]
            held[way][distance, k] = lax.ppermute(held[way][distance - 1, k], "vir", links[way])
            near[way][distance, k] = from_cores(held[way][distance, k])

    shifts = jnp.asarray([distance if way else -distance for distance, way, _ in blocks], jnp.int32)
    sources = jnp.asarray(order, jnp.int32)[lax.rem(spot + shifts + count, count)]
    where = jnp.concatenate([core[None].astype(jnp.int32), sources])
    vir_table = vir_energy.reshape(count, 1, rows)
    own_vir = lax.dynamic_slice_in_dim(vir_energy, place * rows, rows)[:, None]

    density = None
    for number, (distance, way, _) in enumerate(blocks):
        def find(store, k):
            return store[way][distance, k] if (distance, k) in store[way] else store[1 - way][distance, k]

        mine = [find(held, k) for k in range(local)]
        if number == 0:
            theirs = [block[k] for block in own[1:] for k in range(local)]
        else:
            theirs = [find(near, k)[shift] for shift in range(parts - 1) for k in range(local)]
        density = block_step(
            number, parts, where, occ_energy, own_vir, vir_table, own, mine + theirs, density
        )
    return density


def solution(mesh):
    order = ring_order(mesh, "vir")
    parts = mesh.shape["occ"]

    def whole_step(factors, occ_energy, vir_energy):
        return on_device(order, parts, factors, occ_energy, vir_energy)

    return jax.shard_map(
        whole_step,
        mesh=mesh,
        in_specs=(P(("frag", "occ"), "vir", None), P("frag"), P("frag")),
        out_specs=P(("frag", "occ"), "vir", None),
        check_vma=False,
    )
```

```python
import functools

import jax
import jax.numpy as jnp
import numpy as np
from jax import lax
from jax.experimental import pallas as pl
from jax.experimental.pallas import tpu as pltpu
from jax.sharding import PartitionSpec as P

energy_unit = 1.0 / 1024.0


last_cuts = 1

across = (((1,), (1,)), ((), ()))
along = (((1,), (0,)), ((), ()))


def ring_order(mesh, axis):
    devices = mesh.devices
    for name in reversed(mesh.axis_names):
        if name != axis:
            devices = devices[(slice(None),) * mesh.axis_names.index(name) + (0,)]
    count = len(devices)
    spots = [tuple(getattr(device, "coords", ())) for device in devices]
    widths = [len(set(values)) for values in zip(*spots)] if all(spots) else []
    if sorted(widths)[-2:-1] == [2] and sorted(widths)[-1] * 2 == count:
        long = max(range(len(widths)), key=lambda d: widths[d])
        short = [d for d in range(len(widths)) if widths[d] == 2 and d != long][0]
        low = min(spot[short] for spot in spots)
        there = sorted((k for k in range(count) if spots[k][short] == low), key=lambda k: spots[k][long])
        back = sorted((k for k in range(count) if spots[k][short] != low), key=lambda k: -spots[k][long])
        return there + back
    return list(range(count))


def cut_kernel(source, *refs):
    *pieces, sems = refs
    rows = pieces[0].shape[1]
    copies = [
        pltpu.make_async_copy(source.at[:, pl.ds(k * rows, rows), :], piece, sems.at[k])
        for k, piece in enumerate(pieces)
    ]
    for copy in copies:
        copy.start()
    for copy in copies:
        copy.wait()


def cut(source, count):
    local, rows, aux = source.shape
    vmem = pl.BlockSpec(memory_space=pltpu.VMEM)
    return pl.pallas_call(
        cut_kernel,
        out_shape=[jax.ShapeDtypeStruct((local, rows // count, aux), source.dtype)] * count,
        in_specs=[pl.BlockSpec(memory_space=pltpu.HBM)],
        out_specs=[vmem] * count,
        scratch_shapes=[pltpu.SemaphoreType.DMA((count,))],
        compiler_params=pltpu.CompilerParams(vmem_limit_bytes=8 * 1024 * 1024),
        name="cut",
    )(source)


def block_kernel(layout, occ_pairs, own_vir, vir_rows, *refs):
    number, parts, count, steps, tiles, prior, stage = layout
    refs = list(refs)
    own = [refs.pop(0) for _ in range(1 if stage == 2 else parts)]
    if number:
        groups = [[refs.pop(0) for _ in range(count)] for _ in range(1 if stage == 1 else parts)]
    else:
        groups = [[block] for block in own]
    near_amplitude, near_swapped = (refs.pop(0), refs.pop(0)) if stage == 2 else (None, None)
    density_in = refs.pop(0) if prior and stage != 1 else None
    near_out, swapped_out = (refs.pop(0), refs.pop(0)) if stage == 1 else (None, None)
    density_out = refs.pop(0) if stage != 1 else None
    direct = refs.pop(0)
    amplitude, density, out_sem, in_sem = refs if stage != 1 else (near_out, None, None, None)
    local, rows, aux = own[0].shape
    step, depth = aux // tiles, aux // steps
    total = parts * local
    wide = local * rows
    width = sum(piece.shape[1] for piece in groups[0])
    span = local * width
    fresh = [part for part in range(len(groups)) if part or stage != 2]
    starts = {part: (0 if part == 0 else ((parts if stage != 2 else 0) + part - 1) * wide) for part in fresh}

    def tile_copy(start, inward):
        columns = pl.ds(start * step, step)
        if inward:
            return pltpu.make_async_copy(density_in.at[:, :, columns], density.at[:, :, columns], in_sem.at[start])
        return pltpu.make_async_copy(density.at[:, :, columns], density_out.at[:, :, columns], out_sem.at[start])

    if density_in is not None:
        for start in range(tiles):
            tile_copy(start, True).start()

    def stack(arrays):
        return jnp.concatenate(arrays, axis=0) if len(arrays) > 1 else arrays[0]

    def lines(group, columns):
        return [piece[k, :, columns] for k in range(local) for piece in group]

    def depth_step(k, carry):
        columns = pl.ds(pl.multiple_of(k * depth, depth), depth)
        all_rows = stack([block[:, :, columns].reshape(wide, depth) for block in own])
        for part in fresh:
            left = all_rows if part == 0 else all_rows[:wide]
            right = stack(lines(groups[part], columns))
            term = lax.dot_general(left, right, across, preferred_element_type=jnp.float32)
            at = pl.ds(starts[part], left.shape[0])
            direct[at, :] = direct[at, :] + term
        return carry

    direct[...] = jnp.zeros_like(direct)
    lax.fori_loop(0, steps, depth_step, 0)
    vir_pair = own_vir[...] + vir_rows[number][:, :width]

    def tile(row, column, array=direct):
        sums = array[row * rows : (row + 1) * rows, column * width : (column + 1) * width]
        return sums.astype(jnp.bfloat16).astype(jnp.float32)

    for i in range(local):
        for part in fresh:
            for k in range(local):
                j = part * local + k
                divisor = (occ_pairs[i * total + j][:, :width] - vir_pair).astype(jnp.float32) * energy_unit
                straight = tile(starts[part] // rows + i, k)
                crossed = tile(j - local, i, near_swapped) if stage == 2 else tile(j, i)
                here = slice(j * width, (j + 1) * width)
                top = 2.0 * straight - crossed
                amplitude[i * rows : (i + 1) * rows, here] = (top / divisor).astype(jnp.bfloat16)
    if stage == 1:
        swapped_out[...] = direct[wide:, :].astype(jnp.bfloat16)
        return
    if stage == 2:
        amplitude[:, :span] = near_amplitude[...]
    if density_in is not None:
        for start in range(tiles):
            tile_copy(start, True).wait()
    for start in range(tiles):
        columns = slice(start * step, (start + 1) * step)
        factor = stack([line for group in groups for line in lines(group, columns)])
        term = lax.dot_general(amplitude[...], factor, along, preferred_element_type=jnp.float32)
        term = term.reshape(local, rows, step)
        density[:, :, columns] = term if density_in is None else density[:, :, columns] + term
        tile_copy(start, False).start()
    for start in range(tiles):
        tile_copy(start, False).wait()


def block_step(number, energies, own, pieces, density, stage=None, near=()):
    parts = len(own)
    local, rows, aux = own[0].shape
    vmem = pl.BlockSpec(memory_space=pltpu.VMEM)
    hbm = pl.BlockSpec(memory_space=pltpu.HBM)
    groups = 1 if stage == 1 else parts
    own = own[:1] if stage == 2 else own
    operands = [*energies, *own, *pieces, *near]
    specs = [vmem] * len(operands)
    wide = local * rows
    span = local * sum(piece.shape[1] for piece in pieces) // groups if pieces else wide
    tiles = max(k for k in range(1, 4) if aux % (128 * k) == 0)
    steps = max(k for k in range(1, 3) if aux % (128 * k) == 0)
    lines = {None: 2 * parts - 1, 1: parts, 2: parts - 1}[stage]
    prior = density is not None
    layout = (number, parts, len(pieces) // groups, steps, tiles, prior, stage)
    scratch = [pltpu.VMEM((lines * wide, span), jnp.float32)]
    aliases = {}
    if stage == 1:
        out_shape = [
            jax.ShapeDtypeStruct((wide, span), jnp.bfloat16),
            jax.ShapeDtypeStruct(((parts - 1) * wide, span), jnp.bfloat16),
        ]
        out_specs = [vmem, vmem]
    else:
        out_shape = jax.ShapeDtypeStruct((local, rows, aux), jnp.float32)
        out_specs = hbm
        scratch += [
            pltpu.VMEM((wide, parts * span), jnp.bfloat16),
            pltpu.VMEM((local, rows, aux), jnp.float32),
            pltpu.SemaphoreType.DMA((tiles,)),
            pltpu.SemaphoreType.DMA((tiles,)),
        ]
        if prior:
            aliases = {len(operands): 0}
            operands.append(density)
            specs.append(hbm)
    products = lines + (0 if stage == 1 else parts)
    return pl.pallas_call(
        functools.partial(block_kernel, layout),
        out_shape=out_shape,
        in_specs=specs,
        out_specs=out_specs,
        scratch_shapes=scratch,
        input_output_aliases=aliases,
        compiler_params=pltpu.CompilerParams(vmem_limit_bytes=24 * 1024 * 1024),
        cost_estimate=pl.CostEstimate(
            flops=2 * products * wide * span * aux,
            bytes_accessed=2 * (parts * (span + wide) + 4 * wide) * aux,
            transcendentals=0,
        ),
    )(*operands)


def on_device(order, parts, factors, occ_energy, vir_energy):
    local, rows, _ = factors.shape
    count = len(order)
    halves = 2
    core = lax.axis_index("occ")
    place = lax.axis_index("vir")
    onward = [(order[k], order[(k + 1) % count]) for k in range(count)]
    backward = [(target, source) for source, target in onward]
    links = (onward, backward)
    near_core = [[((k + shift) % parts, k) for k in range(parts)] for shift in range(1, parts)]

    first = cut(factors, halves)
    half = rows // halves
    held = [{}, {}]
    own = [factors]
    own += [lax.ppermute(factors, "occ", pairs) for pairs in near_core]
    blocks, shifts, ranges = [], [], []
    for step in range(1, count - 1 + last_cuts):
        at = min(step, count - 1)
        some = half // last_cuts if at == count - 1 else half
        distance = (at + 1) // 2
        begins = [half * ((at - 1 + way) % 2) + some * (step - at) for way in range(2)]
        shifts.append([-distance, distance])
        ranges.append([np.arange(begin, begin + some) for begin in begins])
        for way in range(2):
            source = held[way][at - 2] if at > 2 else first[(at - 1 + way) % 2]
            if some < half:
                source = lax.slice_in_dim(source, some * (step - at), some * (step - at + 1), axis=1)
            held[way][step] = lax.ppermute(source, "vir", links[way])
        arrived = [held[way][step] for way in range(2)]
        block = list(arrived)
        for pairs in near_core:
            for way in range(2):
                block.append(lax.ppermute(arrived[way], "occ", pairs))
        blocks.append(block)

    spots = jnp.asarray([order.index(k) for k in range(count)], jnp.int32)
    away = np.zeros((len(blocks) + 1, rows), np.int32)
    inner = np.tile(np.arange(rows, dtype=np.int32), (len(blocks) + 1, 1))
    for number, (pair, spans) in enumerate(zip(shifts, ranges), 1):
        line = np.concatenate([np.full(len(span), shift) for shift, span in zip(pair, spans)])
        away[number, : len(line)] = line
        inner[number, : len(line)] = np.concatenate(spans)
    sources = jnp.asarray(order, jnp.int32)[(spots[place] + jnp.arange(-count, count, dtype=jnp.int32)) % count]
    energy_table = vir_energy.reshape(count, rows)[sources]
    vir_rows = energy_table[away + count, inner][:, None, :]
    own_vir = lax.dynamic_slice_in_dim(vir_energy, place * rows, rows)[:, None]
    mine_first = jnp.roll(occ_energy, -core * local)
    occ_pairs = (mine_first[:local, None] + mine_first[None, :]).reshape(-1, 1, 1)
    energies = (jnp.broadcast_to(occ_pairs, occ_pairs.shape[:2] + (rows,)), own_vir, vir_rows)

    density = block_step(0, energies, own, [], None)
    for number, block in enumerate(blocks, 1):
        if number < len(blocks):
            density = block_step(number, energies, own, block, density)
        else:
            near = block_step(number, energies, own, block[: len(links)], None, 1)
            density = block_step(number, energies, own, block, density, 2, near)
    return density


def solution(mesh):
    order = ring_order(mesh, "vir")
    parts = mesh.shape["occ"]

    def whole_step(factors, occ_energy, vir_energy):
        return on_device(order, parts, factors, occ_energy, vir_energy)

    return jax.shard_map(
        whole_step,
        mesh=mesh,
        in_specs=(P(("frag", "occ"), "vir", None), P("frag"), P("frag")),
        out_specs=P(("frag", "occ"), "vir", None),
        check_vma=False,
    )
```

```python
import functools

import jax
import jax.numpy as jnp
import numpy as np
from jax import lax
from jax.experimental import pallas as pl
from jax.experimental.pallas import tpu as pltpu
from jax.sharding import PartitionSpec as P

energy_unit = 1.0 / 1024.0


last_cuts = 2
body_steps = 2
body_tiles = 3
last_tiles = 6

across = (((1,), (1,)), ((), ()))
along = (((1,), (0,)), ((), ()))


def ring_order(mesh, axis):
    devices = mesh.devices
    for name in reversed(mesh.axis_names):
        if name != axis:
            devices = devices[(slice(None),) * mesh.axis_names.index(name) + (0,)]
    count = len(devices)
    spots = [tuple(getattr(device, "coords", ())) for device in devices]
    widths = [len(set(values)) for values in zip(*spots)] if all(spots) else []
    if sorted(widths)[-2:-1] == [2] and sorted(widths)[-1] * 2 == count:
        long = max(range(len(widths)), key=lambda d: widths[d])
        short = [d for d in range(len(widths)) if widths[d] == 2 and d != long][0]
        low = min(spot[short] for spot in spots)
        there = sorted((k for k in range(count) if spots[k][short] == low), key=lambda k: spots[k][long])
        back = sorted((k for k in range(count) if spots[k][short] != low), key=lambda k: -spots[k][long])
        return there + back
    return list(range(count))


def cut_kernel(source, *refs):
    *pieces, sems = refs
    slabs, local, rows, slab = pieces[0].shape
    copies = []
    for k, piece in enumerate(pieces):
        for i in range(local):
            for q in range(slabs):
                place = source.at[i, pl.ds(k * rows, rows), pl.ds(q * slab, slab)]
                copies.append(pltpu.make_async_copy(place, piece.at[q, i], sems.at[len(copies)]))
    for copy in copies:
        copy.start()
    for copy in copies:
        copy.wait()


def cut(source, count):
    local, rows, aux = source.shape
    slab = 128 * max(k for k in range(1, 3) if aux % (128 * k) == 0)
    slabs = aux // slab
    vmem = pl.BlockSpec(memory_space=pltpu.VMEM)
    return pl.pallas_call(
        cut_kernel,
        out_shape=[jax.ShapeDtypeStruct((slabs, local, rows // count, slab), source.dtype)] * count,
        in_specs=[pl.BlockSpec(memory_space=pltpu.HBM)],
        out_specs=[vmem] * count,
        scratch_shapes=[pltpu.SemaphoreType.DMA((count * local * slabs,))],
        compiler_params=pltpu.CompilerParams(vmem_limit_bytes=8 * 1024 * 1024),
        name="cut",
    )(source)


def block_kernel(layout, occ_pairs, own_vir, vir_rows, *refs):
    number, parts, owned, count, steps, tiles, prior, stage = layout
    refs = list(refs)
    own = [[refs.pop(0) for _ in range(owned)] for _ in range(1 if stage == 2 else parts)]
    if number:
        groups = [[refs.pop(0) for _ in range(count)] for _ in range(1 if stage == 1 else parts)]
    else:
        groups = own
    near_amplitude, near_swapped, held = (refs.pop(0) for _ in range(3)) if stage == 2 else (None, None, None)
    density_in = refs.pop(0) if prior and stage != 2 else None
    if stage == 1:
        amplitude, swapped_out, density, direct, in_sem = refs
    else:
        density_out, direct, amplitude, density, out_sem, in_sem = refs
    slabs, local, _, slab = own[0][0].shape
    rows = sum(piece.shape[2] for piece in own[0])
    width = sum(piece.shape[2] for piece in groups[0])
    wide, span = local * rows, local * width
    total = parts * local
    step = slabs * slab // tiles
    fresh = [part for part in range(len(groups)) if part or stage != 2]
    starts = {part: (0 if part == 0 else ((parts if stage != 2 else 0) + part - 1) * wide) for part in fresh}

    def tile_copy(start, inward):
        columns = pl.ds(start * step, step)
        if inward:
            return pltpu.make_async_copy(density_in.at[:, :, columns], density.at[:, :, columns], in_sem.at[start])
        return pltpu.make_async_copy(density.at[:, :, columns], density_out.at[:, :, columns], out_sem.at[start])

    if density_in is not None:
        for start in range(tiles):
            tile_copy(start, True).start()

    def stack(arrays, axis=0):
        return jnp.concatenate(arrays, axis=axis) if len(arrays) > 1 else arrays[0]

    def lines(group, first, number_of):
        return [
            stack([piece[first + q, k] for q in range(number_of)], 1) for k in range(local) for piece in group
        ]

    def depth_step(k, carry):
        some = slabs // steps
        all_rows = stack([line for block in own for line in lines(block, k * some, some)])
        for part in fresh:
            left = all_rows if part == 0 else all_rows[:wide]
            right = stack(lines(groups[part], k * some, some))
            term = lax.dot_general(left, right, across, preferred_element_type=jnp.float32)
            at = pl.ds(starts[part], left.shape[0])
            direct[at, :] = direct[at, :] + term
        return carry

    direct[...] = jnp.zeros_like(direct)
    lax.fori_loop(0, steps, depth_step, 0)
    vir_pair = own_vir[...] + vir_rows[number][:, :width]

    def tile(row, column, array=direct):
        sums = array[row * rows : (row + 1) * rows, column * width : (column + 1) * width]
        return sums.astype(jnp.bfloat16).astype(jnp.float32)

    for i in range(local):
        for part in fresh:
            for k in range(local):
                j = part * local + k
                divisor = (occ_pairs[i * total + j][:, :width] - vir_pair).astype(jnp.float32) * energy_unit
                straight = tile(starts[part] // rows + i, k)
                crossed = tile(j - local, i, near_swapped) if stage == 2 else tile(j, i)
                here = slice(j * width, (j + 1) * width)
                top = 2.0 * straight - crossed
                amplitude[i * rows : (i + 1) * rows, here] = (top / divisor).astype(jnp.bfloat16)
    if density_in is not None:
        for start in range(tiles):
            tile_copy(start, True).wait()
    if stage == 1:
        swapped_out[...] = direct[wide:, :].astype(jnp.bfloat16)
        return
    if stage == 2:
        amplitude[:, :span] = near_amplitude[...]
    prior_ref = held if stage == 2 else density if density_in is not None else None
    for start in range(tiles):
        columns = slice(start * step, (start + 1) * step)
        some = slabs // tiles
        factor = stack([line for group in groups for line in lines(group, start * some, some)])
        term = lax.dot_general(amplitude[...], factor, along, preferred_element_type=jnp.float32)
        term = term.reshape(local, rows, step)
        density[:, :, columns] = term if prior_ref is None else prior_ref[:, :, columns] + term
        tile_copy(start, False).start()
    for start in range(tiles):
        tile_copy(start, False).wait()


def block_step(number, energies, own, pieces, density, stage=None, near=()):
    parts = len(own)
    slabs, local, _, slab = own[0][0].shape
    rows = sum(piece.shape[2] for piece in own[0])
    vmem = pl.BlockSpec(memory_space=pltpu.VMEM)
    hbm = pl.BlockSpec(memory_space=pltpu.HBM)
    groups = 1 if stage == 1 else parts
    own = own[:1] if stage == 2 else own
    operands = [*energies, *[piece for block in own for piece in block], *pieces, *near]
    specs = [vmem] * len(operands)
    wide, aux = local * rows, slabs * slab
    span = local * sum(piece.shape[2] for piece in pieces) // groups if pieces else wide
    tiles = max(k for k in range(1, (last_tiles if stage == 2 else body_tiles) + 1) if slabs % k == 0)
    steps = 1 if stage == 1 else max(k for k in range(1, body_steps + 1) if slabs % k == 0)
    lines = {None: 2 * parts - 1, 1: parts, 2: parts - 1}[stage]
    prior = density is not None
    layout = (number, parts, len(own[0]), len(pieces) // groups, steps, tiles, prior, stage)
    scratch = [pltpu.VMEM((lines * wide, span), jnp.float32)]
    out_shape = jax.ShapeDtypeStruct((local, rows, aux), jnp.float32)
    out_specs = hbm
    aliases = {}
    if prior:
        if stage is None:
            aliases = {len(operands): 0}
        operands.append(density)
        specs.append(hbm)
    if stage == 1:
        out_shape = [
            jax.ShapeDtypeStruct((wide, span), jnp.bfloat16),
            jax.ShapeDtypeStruct(((parts - 1) * wide, span), jnp.bfloat16),
            out_shape,
        ]
        out_specs = [vmem] * 3
    else:
        scratch += [
            pltpu.VMEM((wide, parts * span), jnp.bfloat16),
            pltpu.VMEM((local, rows, aux), jnp.float32),
            pltpu.SemaphoreType.DMA((tiles,)),
        ]
    scratch.append(pltpu.SemaphoreType.DMA((tiles,)))
    products = lines + (0 if stage == 1 else parts)
    return pl.pallas_call(
        functools.partial(block_kernel, layout),
        out_shape=out_shape,
        in_specs=specs,
        out_specs=out_specs,
        scratch_shapes=scratch,
        input_output_aliases=aliases,
        compiler_params=pltpu.CompilerParams(vmem_limit_bytes=24 * 1024 * 1024),
        cost_estimate=pl.CostEstimate(
            flops=2 * products * wide * span * aux,
            bytes_accessed=2 * (parts * (span + wide) + 4 * wide) * aux,
            transcendentals=0,
        ),
    )(*operands)


def on_device(order, parts, factors, occ_energy, vir_energy):
    local, rows, _ = factors.shape
    count = len(order)
    halves = 2
    core = lax.axis_index("occ")
    place = lax.axis_index("vir")
    onward = [(order[k], order[(k + 1) % count]) for k in range(count)]
    backward = [(target, source) for source, target in onward]
    links = (onward, backward)
    near_core = [[((k + shift) % parts, k) for k in range(parts)] for shift in range(1, parts)]

    first = cut(factors, halves)
    half = rows // halves
    held = [{}, {}]
    own = [first]
    own += [[lax.ppermute(piece, "occ", pairs) for piece in first] for pairs in near_core]
    blocks, shifts, ranges = [], [], []
    for step in range(1, count - 1 + last_cuts):
        at = min(step, count - 1)
        some = half // last_cuts if at == count - 1 else half
        distance = (at + 1) // 2
        begins = [half * ((at - 1 + way) % 2) + some * (step - at) for way in range(2)]
        shifts.append([-distance, distance])
        ranges.append([np.arange(begin, begin + some) for begin in begins])
        for way in range(2):
            source = held[way][at - 2] if at > 2 else first[(at - 1 + way) % 2]
            if some < half:
                source = lax.slice_in_dim(source, some * (step - at), some * (step - at + 1), axis=2)
            held[way][step] = lax.ppermute(source, "vir", links[way])
        arrived = [held[way][step] for way in range(2)]
        block = list(arrived)
        for pairs in near_core:
            for way in range(2):
                block.append(lax.ppermute(arrived[way], "occ", pairs))
        blocks.append(block)

    spots = jnp.asarray([order.index(k) for k in range(count)], jnp.int32)
    away = np.zeros((len(blocks) + 1, rows), np.int32)
    inner = np.tile(np.arange(rows, dtype=np.int32), (len(blocks) + 1, 1))
    for number, (pair, spans) in enumerate(zip(shifts, ranges), 1):
        line = np.concatenate([np.full(len(span), shift) for shift, span in zip(pair, spans)])
        away[number, : len(line)] = line
        inner[number, : len(line)] = np.concatenate(spans)
    sources = jnp.asarray(order, jnp.int32)[(spots[place] + jnp.arange(-count, count, dtype=jnp.int32)) % count]
    energy_table = vir_energy.reshape(count, rows)[sources]
    vir_rows = energy_table[away + count, inner][:, None, :]
    own_vir = lax.dynamic_slice_in_dim(vir_energy, place * rows, rows)[:, None]
    mine_first = jnp.roll(occ_energy, -core * local)
    occ_pairs = (mine_first[:local, None] + mine_first[None, :]).reshape(-1, 1, 1)
    energies = (jnp.broadcast_to(occ_pairs, occ_pairs.shape[:2] + (rows,)), own_vir, vir_rows)

    density = block_step(0, energies, own, [], None)
    for number, block in enumerate(blocks, 1):
        if number < len(blocks):
            density = block_step(number, energies, own, block, density)
        else:
            near = block_step(number, energies, own, block[: len(links)], density, 1)
            density = block_step(number, energies, own, block, None, 2, near)
    return density


def solution(mesh):
    order = ring_order(mesh, "vir")
    parts = mesh.shape["occ"]

    def whole_step(factors, occ_energy, vir_energy):
        return on_device(order, parts, factors, occ_energy, vir_energy)

    return jax.shard_map(
        whole_step,
        mesh=mesh,
        in_specs=(P(("frag", "occ"), "vir", None), P("frag"), P("frag")),
        out_specs=P(("frag", "occ"), "vir", None),
        check_vma=False,
    )
```

```python
import functools

import jax
import jax.numpy as jnp
import numpy as np
from jax import lax
from jax.experimental import pallas as pl
from jax.experimental.pallas import tpu as pltpu
from jax.sharding import PartitionSpec as P

energy_unit = 1.0 / 1024.0


last_cuts = 2
body_steps = 2
body_tiles = 3
last_tiles = 3

across = (((1,), (1,)), ((), ()))
along = (((1,), (0,)), ((), ()))


def ring_order(mesh, axis):
    devices = mesh.devices
    for name in reversed(mesh.axis_names):
        if name != axis:
            devices = devices[(slice(None),) * mesh.axis_names.index(name) + (0,)]
    count = len(devices)
    spots = [tuple(getattr(device, "coords", ())) for device in devices]
    widths = [len(set(values)) for values in zip(*spots)] if all(spots) else []
    if sorted(widths)[-2:-1] == [2] and sorted(widths)[-1] * 2 == count:
        long = max(range(len(widths)), key=lambda d: widths[d])
        short = [d for d in range(len(widths)) if widths[d] == 2 and d != long][0]
        low = min(spot[short] for spot in spots)
        there = sorted((k for k in range(count) if spots[k][short] == low), key=lambda k: spots[k][long])
        back = sorted((k for k in range(count) if spots[k][short] != low), key=lambda k: -spots[k][long])
        return there + back
    return list(range(count))


def cut_kernel(source, *refs):
    *pieces, sems = refs
    slabs, local, rows, slab = pieces[0].shape
    copies = []
    for k, piece in enumerate(pieces):
        for i in range(local):
            for q in range(slabs):
                place = source.at[i, pl.ds(k * rows, rows), pl.ds(q * slab, slab)]
                copies.append(pltpu.make_async_copy(place, piece.at[q, i], sems.at[len(copies)]))
    for copy in copies:
        copy.start()
    for copy in copies:
        copy.wait()


def cut(source, count):
    local, rows, aux = source.shape
    slab = 128 * max(k for k in range(1, 3) if aux % (128 * k) == 0)
    slabs = aux // slab
    vmem = pl.BlockSpec(memory_space=pltpu.VMEM)
    return pl.pallas_call(
        cut_kernel,
        out_shape=[jax.ShapeDtypeStruct((slabs, local, rows // count, slab), source.dtype)] * count,
        in_specs=[pl.BlockSpec(memory_space=pltpu.HBM)],
        out_specs=[vmem] * count,
        scratch_shapes=[pltpu.SemaphoreType.DMA((count * local * slabs,))],
        compiler_params=pltpu.CompilerParams(vmem_limit_bytes=8 * 1024 * 1024),
        name="cut",
    )(source)


def block_kernel(layout, occ_pairs, own_vir, vir_rows, *refs):
    number, parts, owned, count, steps, tiles, prior, place = layout
    refs = list(refs)
    own = [[refs.pop(0) for _ in range(owned)] for _ in range(parts)]
    groups = [[refs.pop(0) for _ in range(count)] for _ in range(parts)] if number else own
    density_in = refs.pop(0) if prior else None
    if place == "keep":
        density, direct, amplitude, in_sem = refs
    elif place == "held":
        density_out, direct, amplitude, density, out_sem = refs
    else:
        density_out, direct, amplitude, density, out_sem, in_sem = refs
    fetched = prior and place != "held"
    slabs, local, _, slab = own[0][0].shape
    rows = sum(piece.shape[2] for piece in own[0])
    width = sum(piece.shape[2] for piece in groups[0])
    wide = local * rows
    total = parts * local
    step = slabs * slab // tiles
    joined = total * width <= 256

    def tile_copy(start, inward):
        columns = pl.ds(start * step, step)
        if inward:
            return pltpu.make_async_copy(density_in.at[:, :, columns], density.at[:, :, columns], in_sem.at[start])
        return pltpu.make_async_copy(density.at[:, :, columns], density_out.at[:, :, columns], out_sem.at[start])

    if fetched:
        for start in range(tiles):
            tile_copy(start, True).start()

    def stack(arrays, axis=0):
        return jnp.concatenate(arrays, axis=axis) if len(arrays) > 1 else arrays[0]

    def lines(group, first, number_of):
        return [
            stack([piece[first + q, k] for q in range(number_of)], 1) for k in range(local) for piece in group
        ]

    def depth_step(k, carry):
        some = slabs // steps
        all_rows = stack([line for block in own for line in lines(block, k * some, some)])
        if joined:
            right = stack([line for group in groups for line in lines(group, k * some, some)])
            direct[...] = direct[...] + lax.dot_general(all_rows, right, across, preferred_element_type=jnp.float32)
            return carry
        for part in range(parts):
            left = all_rows if part == 0 else all_rows[:wide]
            right = stack(lines(groups[part], k * some, some))
            term = lax.dot_general(left, right, across, preferred_element_type=jnp.float32)
            at = pl.ds(0 if part == 0 else (parts + part - 1) * wide, left.shape[0])
            direct[at, :] = direct[at, :] + term
        return carry

    direct[...] = jnp.zeros_like(direct)
    lax.fori_loop(0, steps, depth_step, 0)
    vir_pair = own_vir[...] + vir_rows[number][:, :width]

    def tile(row, column=None):
        columns = slice(None) if column is None else slice(column * width, (column + 1) * width)
        return direct[row * rows : (row + 1) * rows, columns].astype(jnp.bfloat16).astype(jnp.float32)

    lanes = lax.broadcasted_iota(jnp.int32, (1, total * width), 1) // width
    for i in range(local):
        if joined:
            crossed = None
            for j in range(total):
                line = tile(j) if i == j else pltpu.roll(tile(j), (j - i) % total * width, 1)
                crossed = line if crossed is None else jnp.where(lanes == j, line, crossed)
            pairs = stack([occ_pairs[i * total + j][:, :width] for j in range(total)], 1)
            divisor = (pairs - stack([vir_pair] * total, 1)).astype(jnp.float32) * energy_unit
            amplitude[i * rows : (i + 1) * rows, :] = ((2.0 * tile(i) - crossed) / divisor).astype(jnp.bfloat16)
            continue
        for j in range(total):
            part, k = j // local, j % local
            divisor = (occ_pairs[i * total + j][:, :width] - vir_pair).astype(jnp.float32) * energy_unit
            top = 2.0 * tile(i if part == 0 else (parts + part - 1) * local + i, k) - tile(j, i)
            here = slice(j * width, (j + 1) * width)
            amplitude[i * rows : (i + 1) * rows, here] = (top / divisor).astype(jnp.bfloat16)
    if fetched:
        for start in range(tiles):
            tile_copy(start, True).wait()
    prior_ref = density_in if place == "held" else density if prior else None
    for start in range(tiles):
        columns = slice(start * step, (start + 1) * step)
        some = slabs // tiles
        factor = stack([line for group in groups for line in lines(group, start * some, some)])
        term = lax.dot_general(amplitude[...], factor, along, preferred_element_type=jnp.float32)
        term = term.reshape(local, rows, step)
        density[:, :, columns] = term if prior_ref is None else prior_ref[:, :, columns] + term
        if place != "keep":
            tile_copy(start, False).start()
    if place != "keep":
        for start in range(tiles):
            tile_copy(start, False).wait()


def block_step(number, energies, own, pieces, density, place=None):
    parts = len(own)
    slabs, local, _, slab = own[0][0].shape
    rows = sum(piece.shape[2] for piece in own[0])
    vmem = pl.BlockSpec(memory_space=pltpu.VMEM)
    hbm = pl.BlockSpec(memory_space=pltpu.HBM)
    operands = [*energies, *[piece for block in own for piece in block], *pieces]
    specs = [vmem] * len(operands)
    wide, aux = local * rows, slabs * slab
    span = local * sum(piece.shape[2] for piece in pieces) // parts if pieces else wide
    tiles = max(k for k in range(1, (last_tiles if place == "held" else body_tiles) + 1) if slabs % k == 0)
    steps = max(k for k in range(1, body_steps + 1) if slabs % k == 0)
    joined = parts * span <= 256
    prior = density is not None
    layout = (number, parts, len(own[0]), len(pieces) // parts, steps, tiles, prior, place)
    aliases = {}
    if prior:
        if place is None:
            aliases = {len(operands): 0}
        operands.append(density)
        specs.append(vmem if place == "held" else hbm)
    sums = (parts * wide, parts * span) if joined else ((2 * parts - 1) * wide, span)
    scratch = [pltpu.VMEM(sums, jnp.float32), pltpu.VMEM((wide, parts * span), jnp.bfloat16)]
    if place != "keep":
        scratch += [pltpu.VMEM((local, rows, aux), jnp.float32), pltpu.SemaphoreType.DMA((tiles,))]
    if place != "held":
        scratch.append(pltpu.SemaphoreType.DMA((tiles,)))
    return pl.pallas_call(
        functools.partial(block_kernel, layout),
        out_shape=jax.ShapeDtypeStruct((local, rows, aux), jnp.float32),
        in_specs=specs,
        out_specs=vmem if place == "keep" else hbm,
        scratch_shapes=scratch,
        input_output_aliases=aliases,
        compiler_params=pltpu.CompilerParams(vmem_limit_bytes=24 * 1024 * 1024),
        cost_estimate=pl.CostEstimate(
            flops=2 * (3 * parts - 1) * wide * span * aux,
            bytes_accessed=2 * (parts * (span + wide) + 4 * wide) * aux,
            transcendentals=0,
        ),
    )(*operands)


def on_device(order, parts, factors, occ_energy, vir_energy):
    local, rows, _ = factors.shape
    count = len(order)
    halves = 2
    core = lax.axis_index("occ")
    place = lax.axis_index("vir")
    onward = [(order[k], order[(k + 1) % count]) for k in range(count)]
    backward = [(target, source) for source, target in onward]
    links = (onward, backward)
    near_core = [[((k + shift) % parts, k) for k in range(parts)] for shift in range(1, parts)]

    first = cut(factors, halves)
    half = rows // halves
    held = [{}, {}]
    own = [first]
    own += [[lax.ppermute(piece, "occ", pairs) for piece in first] for pairs in near_core]
    blocks, shifts, ranges = [], [], []
    for step in range(1, count - 1 + last_cuts):
        at = min(step, count - 1)
        some = half // last_cuts if at == count - 1 else half
        distance = (at + 1) // 2
        begins = [half * ((at - 1 + way) % 2) + some * (step - at) for way in range(2)]
        shifts.append([-distance, distance])
        ranges.append([np.arange(begin, begin + some) for begin in begins])
        for way in range(2):
            source = held[way][at - 2] if at > 2 else first[(at - 1 + way) % 2]
            if some < half:
                source = lax.slice_in_dim(source, some * (step - at), some * (step - at + 1), axis=2)
            held[way][step] = lax.ppermute(source, "vir", links[way])
        arrived = [held[way][step] for way in range(2)]
        block = list(arrived)
        for pairs in near_core:
            for way in range(2):
                block.append(lax.ppermute(arrived[way], "occ", pairs))
        blocks.append(block)

    spots = jnp.asarray([order.index(k) for k in range(count)], jnp.int32)
    away = np.zeros((len(blocks) + 1, rows), np.int32)
    inner = np.tile(np.arange(rows, dtype=np.int32), (len(blocks) + 1, 1))
    for number, (pair, spans) in enumerate(zip(shifts, ranges), 1):
        line = np.concatenate([np.full(len(span), shift) for shift, span in zip(pair, spans)])
        away[number, : len(line)] = line
        inner[number, : len(line)] = np.concatenate(spans)
    sources = jnp.asarray(order, jnp.int32)[(spots[place] + jnp.arange(-count, count, dtype=jnp.int32)) % count]
    energy_table = vir_energy.reshape(count, rows)[sources]
    vir_rows = energy_table[away + count, inner][:, None, :]
    own_vir = lax.dynamic_slice_in_dim(vir_energy, place * rows, rows)[:, None]
    mine_first = jnp.roll(occ_energy, -core * local)
    occ_pairs = (mine_first[:local, None] + mine_first[None, :]).reshape(-1, 1, 1)
    energies = (jnp.broadcast_to(occ_pairs, occ_pairs.shape[:2] + (rows,)), own_vir, vir_rows)

    density = block_step(0, energies, own, [], None)
    for number, block in enumerate(blocks, 1):
        place = {len(blocks) - 1: "keep", len(blocks): "held"}.get(number)
        density = block_step(number, energies, own, block, density, place)
    return density


def solution(mesh):
    order = ring_order(mesh, "vir")
    parts = mesh.shape["occ"]

    def whole_step(factors, occ_energy, vir_energy):
        return on_device(order, parts, factors, occ_energy, vir_energy)

    return jax.shard_map(
        whole_step,
        mesh=mesh,
        in_specs=(P(("frag", "occ"), "vir", None), P("frag"), P("frag")),
        out_specs=P(("frag", "occ"), "vir", None),
        check_vma=False,
    )
```

```python
import functools

import jax
import jax.numpy as jnp
import numpy as np
from jax import lax
from jax.experimental import pallas as pl
from jax.experimental.pallas import tpu as pltpu
from jax.sharding import PartitionSpec as P

energy_unit = 1.0 / 1024.0


last_cuts = 2
body_steps = 2
body_tiles = 3
last_tiles = 4

across = (((1,), (1,)), ((), ()))
along = (((1,), (0,)), ((), ()))


def ring_order(mesh, axis):
    devices = mesh.devices
    for name in reversed(mesh.axis_names):
        if name != axis:
            devices = devices[(slice(None),) * mesh.axis_names.index(name) + (0,)]
    count = len(devices)
    spots = [tuple(getattr(device, "coords", ())) for device in devices]
    widths = [len(set(values)) for values in zip(*spots)] if all(spots) else []
    if sorted(widths)[-2:-1] == [2] and sorted(widths)[-1] * 2 == count:
        long = max(range(len(widths)), key=lambda d: widths[d])
        short = [d for d in range(len(widths)) if widths[d] == 2 and d != long][0]
        low = min(spot[short] for spot in spots)
        there = sorted((k for k in range(count) if spots[k][short] == low), key=lambda k: spots[k][long])
        back = sorted((k for k in range(count) if spots[k][short] != low), key=lambda k: -spots[k][long])
        return there + back
    return list(range(count))


def cut_kernel(source, *refs):
    *pieces, sems = refs
    slabs, local, rows, slab = pieces[0].shape
    copies = []
    for k, piece in enumerate(pieces):
        for i in range(local):
            for q in range(slabs):
                place = source.at[i, pl.ds(k * rows, rows), pl.ds(q * slab, slab)]
                copies.append(pltpu.make_async_copy(place, piece.at[q, i], sems.at[len(copies)]))
    for copy in copies:
        copy.start()
    for copy in copies:
        copy.wait()


def cut(source, count):
    local, rows, aux = source.shape
    slab = 128 * max(k for k in range(1, 3) if aux % (128 * k) == 0)
    slabs = aux // slab
    vmem = pl.BlockSpec(memory_space=pltpu.VMEM)
    return pl.pallas_call(
        cut_kernel,
        out_shape=[jax.ShapeDtypeStruct((slabs, local, rows // count, slab), source.dtype)] * count,
        in_specs=[pl.BlockSpec(memory_space=pltpu.HBM)],
        out_specs=[vmem] * count,
        scratch_shapes=[pltpu.SemaphoreType.DMA((count * local * slabs,))],
        compiler_params=pltpu.CompilerParams(vmem_limit_bytes=8 * 1024 * 1024),
        name="cut",
    )(source)


def block_kernel(layout, occ_pairs, own_vir, vir_rows, *refs):
    number, parts, owned, count, steps, tiles, prior, stage = layout
    refs = list(refs)
    own = [[refs.pop(0) for _ in range(owned)] for _ in range(1 if stage == 2 else parts)]
    if number:
        groups = [[refs.pop(0) for _ in range(count)] for _ in range(1 if stage == 1 else parts)]
    else:
        groups = own
    near_amplitude, near_swapped, held = (refs.pop(0) for _ in range(3)) if stage == 2 else (None, None, None)
    density_in = refs.pop(0) if prior and stage != 2 else None
    if stage == 1:
        amplitude, swapped_out, density, direct, in_sem = refs
    else:
        density_out, direct, amplitude, density, out_sem, in_sem = refs
    slabs, local, _, slab = own[0][0].shape
    rows = sum(piece.shape[2] for piece in own[0])
    width = sum(piece.shape[2] for piece in groups[0])
    wide, span = local * rows, local * width
    total = parts * local
    step = slabs * slab // tiles
    fresh = [part for part in range(len(groups)) if part or stage != 2]
    starts = {part: (0 if part == 0 else ((parts if stage != 2 else 0) + part - 1) * wide) for part in fresh}

    def tile_copy(start, inward):
        columns = pl.ds(start * step, step)
        if inward:
            return pltpu.make_async_copy(density_in.at[:, :, columns], density.at[:, :, columns], in_sem.at[start])
        return pltpu.make_async_copy(density.at[:, :, columns], density_out.at[:, :, columns], out_sem.at[start])

    if density_in is not None:
        for start in range(tiles):
            tile_copy(start, True).start()

    def stack(arrays, axis=0):
        return jnp.concatenate(arrays, axis=axis) if len(arrays) > 1 else arrays[0]

    def lines(group, first, number_of):
        return [
            stack([piece[first + q, k] for q in range(number_of)], 1) for k in range(local) for piece in group
        ]

    def depth_step(k, carry):
        some = slabs // steps
        all_rows = stack([line for block in own for line in lines(block, k * some, some)])
        for part in fresh:
            left = all_rows if part == 0 else all_rows[:wide]
            right = stack(lines(groups[part], k * some, some))
            term = lax.dot_general(left, right, across, preferred_element_type=jnp.float32)
            at = pl.ds(starts[part], left.shape[0])
            direct[at, :] = direct[at, :] + term
        return carry

    direct[...] = jnp.zeros_like(direct)
    lax.fori_loop(0, steps, depth_step, 0)
    vir_pair = own_vir[...] + vir_rows[number][:, :width]

    lanes = lax.broadcasted_iota(jnp.int32, (1, local * width), 1) // width
    for i in range(local):
        for part in fresh:
            straight = direct[starts[part] + i * rows : starts[part] + (i + 1) * rows, :]
            straight = straight.astype(jnp.bfloat16).astype(jnp.float32)
            crossed = None
            for k in range(local):
                j = part * local + k
                array, row = (near_swapped, j - local) if stage == 2 else (direct, j)
                line = array[row * rows : (row + 1) * rows, :].astype(jnp.bfloat16).astype(jnp.float32)
                if k != i:
                    line = pltpu.roll(line, (k - i) % local * width, 1)
                crossed = line if crossed is None else jnp.where(lanes == k, line, crossed)
            pair = [occ_pairs[i * total + part * local + k][:, :width] for k in range(local)]
            divisor = (stack(pair, 1) - stack([vir_pair] * local, 1)).astype(jnp.float32) * energy_unit
            here = slice(part * local * width, (part + 1) * local * width)
            amplitude[i * rows : (i + 1) * rows, here] = ((2.0 * straight - crossed) / divisor).astype(jnp.bfloat16)
    if density_in is not None:
        for start in range(tiles):
            tile_copy(start, True).wait()
    if stage == 1:
        swapped_out[...] = direct[wide:, :].astype(jnp.bfloat16)
        return
    if stage == 2:
        amplitude[:, :span] = near_amplitude[...]
    prior_ref = held if stage == 2 else density if density_in is not None else None
    for start in range(tiles):
        columns = slice(start * step, (start + 1) * step)
        some = slabs // tiles
        factor = stack([line for group in groups for line in lines(group, start * some, some)])
        term = lax.dot_general(amplitude[...], factor, along, preferred_element_type=jnp.float32)
        term = term.reshape(local, rows, step)
        density[:, :, columns] = term if prior_ref is None else prior_ref[:, :, columns] + term
        tile_copy(start, False).start()
    for start in range(tiles):
        tile_copy(start, False).wait()


def block_step(number, energies, own, pieces, density, stage=None, near=()):
    parts = len(own)
    slabs, local, _, slab = own[0][0].shape
    rows = sum(piece.shape[2] for piece in own[0])
    vmem = pl.BlockSpec(memory_space=pltpu.VMEM)
    hbm = pl.BlockSpec(memory_space=pltpu.HBM)
    groups = 1 if stage == 1 else parts
    own = own[:1] if stage == 2 else own
    operands = [*energies, *[piece for block in own for piece in block], *pieces, *near]
    specs = [vmem] * len(operands)
    wide, aux = local * rows, slabs * slab
    span = local * sum(piece.shape[2] for piece in pieces) // groups if pieces else wide
    tiles = max(k for k in range(1, (last_tiles if stage == 2 else body_tiles) + 1) if slabs % k == 0)
    steps = 1 if stage == 1 else max(k for k in range(1, body_steps + 1) if slabs % k == 0)
    lines = {None: 2 * parts - 1, 1: parts, 2: parts - 1}[stage]
    prior = density is not None
    layout = (number, parts, len(own[0]), len(pieces) // groups, steps, tiles, prior, stage)
    scratch = [pltpu.VMEM((lines * wide, span), jnp.float32)]
    out_shape = jax.ShapeDtypeStruct((local, rows, aux), jnp.float32)
    out_specs = hbm
    aliases = {}
    if prior:
        if stage is None:
            aliases = {len(operands): 0}
        operands.append(density)
        specs.append(hbm)
    if stage == 1:
        out_shape = [
            jax.ShapeDtypeStruct((wide, span), jnp.bfloat16),
            jax.ShapeDtypeStruct(((parts - 1) * wide, span), jnp.bfloat16),
            out_shape,
        ]
        out_specs = [vmem] * 3
    else:
        scratch += [
            pltpu.VMEM((wide, parts * span), jnp.bfloat16),
            pltpu.VMEM((local, rows, aux), jnp.float32),
            pltpu.SemaphoreType.DMA((tiles,)),
        ]
    scratch.append(pltpu.SemaphoreType.DMA((tiles,)))
    products = lines + (0 if stage == 1 else parts)
    return pl.pallas_call(
        functools.partial(block_kernel, layout),
        out_shape=out_shape,
        in_specs=specs,
        out_specs=out_specs,
        scratch_shapes=scratch,
        input_output_aliases=aliases,
        compiler_params=pltpu.CompilerParams(vmem_limit_bytes=24 * 1024 * 1024),
        cost_estimate=pl.CostEstimate(
            flops=2 * products * wide * span * aux,
            bytes_accessed=2 * (parts * (span + wide) + 4 * wide) * aux,
            transcendentals=0,
        ),
    )(*operands)


def on_device(order, parts, factors, occ_energy, vir_energy):
    local, rows, _ = factors.shape
    count = len(order)
    halves = 2
    core = lax.axis_index("occ")
    place = lax.axis_index("vir")
    onward = [(order[k], order[(k + 1) % count]) for k in range(count)]
    backward = [(target, source) for source, target in onward]
    links = (onward, backward)
    near_core = [[((k + shift) % parts, k) for k in range(parts)] for shift in range(1, parts)]

    first = cut(factors, halves)
    half = rows // halves
    held = [{}, {}]
    own = [first]
    own += [[lax.ppermute(piece, "occ", pairs) for piece in first] for pairs in near_core]
    blocks, shifts, ranges = [], [], []
    for step in range(1, count - 1 + last_cuts):
        at = min(step, count - 1)
        some = half // last_cuts if at == count - 1 else half
        distance = (at + 1) // 2
        begins = [half * ((at - 1 + way) % 2) + some * (step - at) for way in range(2)]
        shifts.append([-distance, distance])
        ranges.append([np.arange(begin, begin + some) for begin in begins])
        for way in range(2):
            source = held[way][at - 2] if at > 2 else first[(at - 1 + way) % 2]
            if some < half:
                source = lax.slice_in_dim(source, some * (step - at), some * (step - at + 1), axis=2)
            held[way][step] = lax.ppermute(source, "vir", links[way])
        arrived = [held[way][step] for way in range(2)]
        block = list(arrived)
        for pairs in near_core:
            for way in range(2):
                block.append(lax.ppermute(arrived[way], "occ", pairs))
        blocks.append(block)

    spots = jnp.asarray([order.index(k) for k in range(count)], jnp.int32)
    away = np.zeros((len(blocks) + 1, rows), np.int32)
    inner = np.tile(np.arange(rows, dtype=np.int32), (len(blocks) + 1, 1))
    for number, (pair, spans) in enumerate(zip(shifts, ranges), 1):
        line = np.concatenate([np.full(len(span), shift) for shift, span in zip(pair, spans)])
        away[number, : len(line)] = line
        inner[number, : len(line)] = np.concatenate(spans)
    sources = jnp.asarray(order, jnp.int32)[(spots[place] + jnp.arange(-count, count, dtype=jnp.int32)) % count]
    energy_table = vir_energy.reshape(count, rows)[sources]
    vir_rows = energy_table[away + count, inner][:, None, :]
    own_vir = lax.dynamic_slice_in_dim(vir_energy, place * rows, rows)[:, None]
    mine_first = jnp.roll(occ_energy, -core * local)
    occ_pairs = (mine_first[:local, None] + mine_first[None, :]).reshape(-1, 1, 1)
    energies = (jnp.broadcast_to(occ_pairs, occ_pairs.shape[:2] + (rows,)), own_vir, vir_rows)

    density = block_step(0, energies, own, [], None)
    for number, block in enumerate(blocks, 1):
        if number < len(blocks):
            density = block_step(number, energies, own, block, density)
        else:
            near = block_step(number, energies, own, block[: len(links)], density, 1)
            density = block_step(number, energies, own, block, None, 2, near)
    return density


def solution(mesh):
    order = ring_order(mesh, "vir")
    parts = mesh.shape["occ"]

    def whole_step(factors, occ_energy, vir_energy):
        return on_device(order, parts, factors, occ_energy, vir_energy)

    return jax.shard_map(
        whole_step,
        mesh=mesh,
        in_specs=(P(("frag", "occ"), "vir", None), P("frag"), P("frag")),
        out_specs=P(("frag", "occ"), "vir", None),
        check_vma=False,
    )
```
